256 devices in a mesh: ctx: 32 (over z, y), tp: 8 (over x, core).
Axes of the slice: x: 4, y: 4, z: 8, core: 2. Of those that a mesh axis runs over, the one named last changes fastest.
Arguments:
- queries: bfloat16 [8192, 64, 128], P('ctx', 'tp'), may hold values from -48 to 48
- keys: bfloat16 [8192, 8, 128], P('ctx', 'tp'), may hold values from -3 to 3
- values: bfloat16 [8192, 8, 128], P('ctx', 'tp'), may hold values from -6 to 6
- segment_ids: int32 [8192], P('ctx'), may hold values from 0 to 7, never falling along the last dimension, each value on 1 to 5120 neighbouring positions
Outputs:
- attended: bfloat16 [8192, 8192], P(('ctx', 'tp'))
The draws below stay inside these ranges and needn't reach their ends.
Inputs may be any that keep to these rules, and one draw needn't show every extreme that they name: `segment_ids`: ids never fall along the tokens; each document holds 1 to 5120 tokens, and one holds exactly 5120.
All inputs are finite; a program needn't handle non-finite values.
Results may differ from the reference program's by a relative error of at most 0.003.
Values may be sent and summed in bfloat16 or wider, within the bound.
No kernel may reach another device: no remote copies, remote signals or barrier semaphores. Data moves between devices by JAX's collectives and lax.ppermute only.
A program may use at most 64 MiB of HBM per device.

```python
import math
import jax
import jax.numpy as jnp
import numpy as np
from jax import lax

QUERY_HEADS = 64
KEY_VALUE_HEADS = 8
HEAD_SIZE = 128
DOCS = 8
PACK_TOKENS = 8192
MOST = 5120


def paired_draw(key):
    base = jax.random.fold_in(key, 4242)
    key_random_keys, key_query = jax.random.split(base, 2)
    keys = jnp.clip(jax.random.normal(key_random_keys, (PACK_TOKENS, KEY_VALUE_HEADS, HEAD_SIZE), jnp.float32), -3.0, 3.0)
    queries = jnp.clip(2.5 * jax.random.normal(key_query, (PACK_TOKENS, QUERY_HEADS, HEAD_SIZE), jnp.float32), -12.0, 12.0)
    return (queries.astype(jnp.bfloat16), keys.astype(jnp.bfloat16))


def draw_queries(key, part):
    return paired_draw(key)[0]


def draw_keys(key, part):
    return paired_draw(key)[1]


def shard_levels(own_key, extent, cuts, least, high):
    loudness, own = 1.0, jax.random.fold_in(own_key, 6)
    for position, shards_of in cuts:
        heights = jnp.exp(jax.random.uniform(jax.random.fold_in(own, position), (shards_of,), jnp.float32, least / len(cuts), high / len(cuts)))
        loudness = loudness * jnp.repeat(heights, extent[position] // shards_of).reshape([-1 if axis == position else 1 for axis in range(len(extent))])
    return loudness


def length_profile(count, total, most, lean):
    weights = [(1 << 20) // math.isqrt(standing ** lean) + 1 for standing in range(2, count + 1)]
    spare, given = total - most - (count - 1), [1] * (count - 1)
    while spare > 0:
        free = [i for i in range(count - 1) if given[i] < most]
        mass, remaining = sum([weights[i] for i in free]), spare
        for i in free:
            addition = min(most - given[i], max(1, remaining * weights[i] // mass), spare)
            given[i] = given[i] + addition
            spare = spare - addition
    return np.array([most] + given)


def uneven(rng, amount, total, limit, skew):
    if amount == 2:
        one = jax.random.randint(rng, (), max(1, total - limit), min(limit, total - 1) + 1)
        return jnp.stack([one, total - one])
    lengths = jnp.asarray(length_profile(amount, total, limit, skew), jnp.int32)
    couples = (amount - 1) // 2
    donor, taker = lengths[1:1 + 2 * couples:2], lengths[2:2 + 2 * couples:2]
    room = jnp.minimum(donor - 1, limit - taker)
    moved = jax.random.randint(jax.random.fold_in(rng, 1), (couples,), 0, 1 << 20) % (room + 1)
    lengths = lengths.at[1:1 + 2 * couples:2].set(donor - moved).at[2:2 + 2 * couples:2].set(taker + moved)
    return lengths[jax.random.permutation(jax.random.fold_in(rng, 2), amount)]


def scatter_about(key, extent, deviation, limit, shards=(), kind=jnp.bfloat16):
    gain = shard_levels(key, extent, shards, -0.22, 0.18) if shards else 1.0
    values = jax.random.normal(key, extent, jnp.float32) * deviation * gain
    return jnp.minimum(jnp.maximum(values, -limit), limit).astype(kind)


def setup_inputs(seed: int = 0) -> dict:
    arg_keys = jax.random.split(jax.random.key(seed), 5)
    return {
        "queries": draw_queries(jax.random.fold_in(arg_keys[4], 71), 0),
        "keys": draw_keys(jax.random.fold_in(arg_keys[4], 71), 0),
        "values": scatter_about(arg_keys[2], (PACK_TOKENS, KEY_VALUE_HEADS, HEAD_SIZE), 1.0, 6.0, ((0, 32), (1, 8))),
        "segment_ids": jnp.searchsorted(jnp.cumsum(uneven(arg_keys[3], DOCS, PACK_TOKENS, MOST, 2)), jnp.arange(PACK_TOKENS), side="right").astype(jnp.int32),
    }


def reference(queries, keys, values, segment_ids):
    tokens, heads, head = queries.shape
    groups = keys.shape[1]
    per_group = heads // groups
    block = math.gcd(tokens, 512)
    positions = jnp.arange(tokens, dtype=jnp.int32)
    scale = 1.0 / math.sqrt(head)

    def one_block(index):
        first = (index * block).astype(jnp.int32)
        query_rows = lax.dynamic_slice_in_dim(queries, first, block, 0).reshape(block, groups, per_group, head)
        seg_rows = lax.dynamic_slice_in_dim(segment_ids, first, block, 0)
        pos_rows = first + jnp.arange(block, dtype=jnp.int32)
        allowed = (seg_rows[:, None] == segment_ids[None, :]) & (positions[None, :] <= pos_rows[:, None])

        def one_group(group):
            query_group = lax.dynamic_index_in_dim(query_rows, group, 1, keepdims=False).astype(jnp.float32)
            key_group = lax.dynamic_index_in_dim(keys, group, 1, keepdims=False).astype(jnp.float32)
            value_group = lax.dynamic_index_in_dim(values, group, 1, keepdims=False).astype(jnp.float32)
            scores = jnp.einsum('tgd,pd->gtp', query_group, key_group) * scale
            scores = jnp.where(allowed[None], scores, -1e+30)
            top = lax.optimization_barrier(jnp.max(scores, axis=-1))
            weights = jnp.where(allowed[None], jnp.exp(scores - top[..., None]), 0.0)
            total = lax.optimization_barrier(jnp.sum(weights, axis=-1))
            rounded = lax.optimization_barrier(weights.astype(jnp.bfloat16)).astype(jnp.float32)
            mixed = jnp.einsum('gtp,pd->gtd', rounded, value_group)
            return mixed / total[..., None]
        result = lax.map(one_group, jnp.arange(groups, dtype=jnp.int32))
        return jnp.transpose(result, (2, 0, 1, 3)).reshape(block, heads * head).astype(jnp.bfloat16)
    output = lax.map(one_block, jnp.arange(tokens // block, dtype=jnp.int32))
    return output.reshape(tokens, heads * head)
```

```python
import functools
import math

import jax
import jax.numpy as jnp
from jax import lax
from jax.experimental import pallas as pl
from jax.experimental.pallas import tpu as pltpu
from jax.sharding import PartitionSpec as P

ROWS = 256
HEADS = 8
HEAD = 128
TILE = 32
TILES = ROWS // TILE
COLS = TILE * HEADS
FACTOR = math.log2(math.e) / math.sqrt(HEAD)
NEG = -1e30
PAYLOAD = 2 * ROWS + 16


def scores_of(keys, q_ref, tile):
    q = q_ref[pl.ds(tile * COLS, COLS), :]
    return lax.dot_general(keys, q, (((1,), (1,)), ((), ())), preferred_element_type=jnp.float32)


def fold(scores, values_t, tile, m_ref, l_ref, acc_ref):
    old = m_ref[tile]
    top = jnp.maximum(old, jnp.max(scores, axis=0, keepdims=True))
    weights = jnp.exp2((scores - top) * FACTOR)
    decay = jnp.exp2((old - top) * FACTOR)
    l_ref[tile] = l_ref[tile] * decay + jnp.sum(weights, axis=0, keepdims=True)
    m_ref[tile] = top
    mixed = jnp.dot(values_t, weights.astype(jnp.bfloat16), preferred_element_type=jnp.float32)
    acc_ref[tile] = acc_ref[tile] * decay + mixed


def attention_kernel(meta_ref, q_ref, kv_ref, low_ref, own_ref, out_ref, m_ref, l_ref, acc_ref):
    here, doc, prefix = meta_ref[0], meta_ref[1], meta_ref[2]
    blocks = kv_ref.shape[0]
    ids = kv_ref[:, 2 * ROWS : 2 * ROWS + 2, :].astype(jnp.float32)
    begin = jnp.sum((ids < doc.astype(jnp.float32)).astype(jnp.int32))
    first = begin // ROWS

    def block_of(index):
        keys = kv_ref[index, 0:ROWS, :]
        values_t = jnp.concatenate([kv_ref[index, ROWS : ROWS + 128, :], kv_ref[index, ROWS + 128 : 2 * ROWS, :]], axis=1)
        return keys, values_t

    keys, values_t = block_of(here)
    for tile in range(TILES):
        row = lax.broadcasted_iota(jnp.int32, (ROWS, COLS), 0)
        token = tile * TILE + lax.rem(lax.broadcasted_iota(jnp.int32, (1, COLS), 1), TILE)
        allowed = (row >= low_ref[tile]) & (row <= token)
        scores = jnp.where(allowed, scores_of(keys, q_ref, tile), NEG)
        top = jnp.max(scores, axis=0, keepdims=True)
        weights = jnp.exp2((scores - top) * FACTOR)
        m_ref[tile] = top
        l_ref[tile] = jnp.sum(weights, axis=0, keepdims=True)
        acc_ref[tile] = jnp.dot(values_t, weights.astype(jnp.bfloat16), preferred_element_type=jnp.float32)

    def one_block(index, _):
        whole = (begin <= index * ROWS) & (prefix == ROWS)

        @pl.when(whole)
        def _():
            keys, values_t = block_of(index)
            for tile in range(TILES):
                fold(scores_of(keys, q_ref, tile), values_t, tile, m_ref, l_ref, acc_ref)

        @pl.when(jnp.logical_not(whole))
        def _():
            def one_tile(tile, _):
                @pl.when(tile * TILE < prefix)
                def _():
                    keys, values_t = block_of(index)
                    row = index * ROWS + lax.broadcasted_iota(jnp.int32, (ROWS, COLS), 0)
                    low = jnp.where(own_ref[tile] == 1, begin, blocks * ROWS)
                    scores = jnp.where(row >= low, scores_of(keys, q_ref, tile), NEG)
                    fold(scores, values_t, tile, m_ref, l_ref, acc_ref)

                return 0

            lax.fori_loop(0, TILES, one_tile, 0)

        return 0

    lax.fori_loop(first, here, one_block, 0)

    for tile in range(TILES):
        done = (acc_ref[tile] * (1.0 / l_ref[tile])).T.astype(jnp.bfloat16)
        for head in range(HEADS):
            out_ref[tile, :, head * HEAD : (head + 1) * HEAD] = done[head * TILE : (head + 1) * TILE, :]


def attend(meta, q, kv, low, own):
    vmem = pl.BlockSpec(memory_space=pltpu.VMEM)
    return pl.pallas_call(
        attention_kernel,
        out_shape=jax.ShapeDtypeStruct((TILES, TILE, HEADS * HEAD), jnp.bfloat16),
        in_specs=[pl.BlockSpec(memory_space=pltpu.SMEM), vmem, vmem, vmem, vmem],
        out_specs=vmem,
        scratch_shapes=[
            pltpu.VMEM((TILES, 1, COLS), jnp.float32),
            pltpu.VMEM((TILES, 1, COLS), jnp.float32),
            pltpu.VMEM((TILES, HEAD, COLS), jnp.float32),
        ],
        name="attention",
    )(meta, q, kv, low, own)


def local(queries, keys, values, segment_ids):
    here = lax.axis_index("ctx").astype(jnp.int32)
    k = keys.reshape(ROWS, HEAD)
    vt = values.reshape(2, 128, HEAD).transpose(0, 2, 1).reshape(ROWS, 128)
    ids = jnp.pad(segment_ids.reshape(2, 128).astype(jnp.bfloat16), ((0, 14), (0, 0)))
    payload = jnp.concatenate([k, vt, ids], axis=0)
    kv = lax.all_gather(payload, "ctx", axis=0, tiled=False)

    q = queries.reshape(TILES, TILE, HEADS, HEAD).transpose(0, 2, 1, 3).reshape(TILES * COLS, HEAD)
    doc = segment_ids[0]
    own = (segment_ids == doc).astype(jnp.int32)
    meta = jnp.stack([here, doc, jnp.sum(own)])
    low = jnp.sum((segment_ids[None, :] < segment_ids[:, None]).astype(jnp.int32), axis=1)
    spread = lambda a: jnp.broadcast_to(a.reshape(TILES, 1, 1, TILE), (TILES, 1, HEADS, TILE)).reshape(TILES, 1, COLS)
    out = attend(meta, q, kv, spread(low), spread(own))
    out = lax.all_to_all(out, "tp", split_axis=0, concat_axis=0, tiled=True)
    return out.transpose(1, 0, 2).reshape(TILE, TILES * HEADS * HEAD)


def solution(mesh):
    in_specs = (P("ctx", "tp", None), P("ctx", "tp", None), P("ctx", "tp", None), P("ctx"))
    out_specs = P(("ctx", "tp"), None)
    return jax.shard_map(local, mesh=mesh, in_specs=in_specs, out_specs=out_specs, check_vma=False)
```

```python
import functools
import math

import jax
import jax.numpy as jnp
from jax import lax
from jax.experimental import pallas as pl
from jax.experimental.pallas import tpu as pltpu
from jax.sharding import PartitionSpec as P

Z, Y = 8, 4
ROWS = 256
HEADS = 8
HEAD = 128
TILE = 32
TILES = ROWS // TILE
COLS = TILE * HEADS
FACTOR = math.log2(math.e) / math.sqrt(HEAD)
NEG = -1e30
PART_A = 192
PART_B = 2 * ROWS - PART_A
IDS = 16
OFFSETS = (0, 1, 3, 2)
BUFFERS = 4


def prepare_kernel(k_ref, v_ref, ids_ref, a_ref, b_ref):
    a_ref[0:PART_A, :] = k_ref[0:PART_A, :]
    a_ref[PART_A : PART_A + 8, :] = jnp.zeros((8, 128), jnp.bfloat16)
    a_ref[PART_A + 8 : PART_A + 16, :] = jnp.zeros((8, 128), jnp.bfloat16)
    a_ref[PART_A : PART_A + 2, :] = ids_ref[...].astype(jnp.float32).astype(jnp.bfloat16)
    b_ref[0 : ROWS - PART_A, :] = k_ref[PART_A:ROWS, :]
    for half in range(2):
        at = ROWS - PART_A + half * 128
        v = v_ref[half * 128 : (half + 1) * 128, :].astype(jnp.float32)
        b_ref[at : at + 128, :] = v.T.astype(jnp.bfloat16)


def prepare(k, v, ids):
    vmem = pl.BlockSpec(memory_space=pltpu.VMEM)
    return pl.pallas_call(
        prepare_kernel,
        out_shape=(
            jax.ShapeDtypeStruct((PART_A + IDS, 128), jnp.bfloat16),
            jax.ShapeDtypeStruct((PART_B, 128), jnp.bfloat16),
        ),
        in_specs=[vmem] * 3,
        out_specs=(vmem, vmem),
        name="prepare",
    )(k, v, ids)


def fold_chunk(first_slot, blocks, cuts, q_ref, kv_ref, m_ref, l_ref, acc_ref, s_ref, top_ref):
    length = blocks * ROWS
    carried = {}

    def scores(tile):
        q = q_ref[tile * COLS : (tile + 1) * COLS, :]
        part = None
        for g in range(blocks):
            keys = kv_ref[first_slot + g, 0:ROWS, :]
            s = lax.dot_general(keys, q, (((1,), (1,)), ((), ())), preferred_element_type=jnp.float32)
            if cuts is not None:
                row = lax.broadcasted_iota(jnp.int32, (ROWS, COLS), 0)
                s = jnp.where(row >= cuts[g], s, NEG)
            s_ref[tile % BUFFERS, g * ROWS : (g + 1) * ROWS, :] = s
            top = jnp.max(s.reshape(ROWS // 8, 8, COLS), axis=0)
            part = top if part is None else jnp.maximum(part, top)
        top_ref[tile % BUFFERS] = part

    def tops(tile):
        old = m_ref[tile]
        top = jnp.maximum(old, jnp.max(top_ref[tile % BUFFERS], axis=0, keepdims=True))
        m_ref[tile] = top
        carried[tile] = top, jnp.exp2((old - top) * FACTOR)

    def mix(tile):
        top, decay = carried.pop(tile)
        weights = jnp.exp2((s_ref[tile % BUFFERS, 0:length, :] - top) * FACTOR)
        values_t = jnp.concatenate(
            [kv_ref[first_slot + g, ROWS + h * 128 : ROWS + (h + 1) * 128, :] for g in range(blocks) for h in range(2)],
            axis=1,
        )
        mixed = jnp.dot(values_t, weights.astype(jnp.bfloat16), preferred_element_type=jnp.float32)
        l_ref[tile] = l_ref[tile] * decay + jnp.sum(weights.reshape(length // 8, 8, COLS), axis=0)
        acc_ref[tile] = acc_ref[tile] * decay + mixed

    for step in range(TILES + 2):
        if step < TILES:
            scores(step)
        if 0 <= step - 1 < TILES:
            tops(step - 1)
        if 0 <= step - 2 < TILES:
            mix(step - 2)


def own_block(q_ref, k_of, vt_of, low_ref, own_ref, m_ref, l_ref, acc_ref):
    row = lax.broadcasted_iota(jnp.int32, (ROWS, COLS), 0)
    column = lax.broadcasted_iota(jnp.int32, (1, COLS), 1)
    for tile in range(TILES):
        token = tile * TILE + lax.rem(column, TILE)
        q = q_ref[tile * COLS : (tile + 1) * COLS, :]
        s = lax.dot_general(k_of(), q, (((1,), (1,)), ((), ())), preferred_element_type=jnp.float32)
        s = jnp.where((row >= low_ref[tile]) & (row <= token), s, NEG)
        top = jnp.max(s, axis=0, keepdims=True)
        weights = jnp.exp2((s - top) * FACTOR)
        l_ref[tile] = jnp.sum(weights.reshape(ROWS // 8, 8, COLS), axis=0)
        acc_ref[tile] = jnp.dot(vt_of(), weights.astype(jnp.bfloat16), preferred_element_type=jnp.float32)
        m_ref[tile] = jnp.where(own_ref[tile] == 1, top, -NEG)


def stage_kernel(rows, first, last, *refs):
    refs = list(refs)
    meta_ref, q_ref = refs.pop(0), refs.pop(0)
    a_refs = [refs.pop(0) for _ in rows]
    b_refs = [refs.pop(0) for _ in OFFSETS]
    if first:
        low_ref, own_ref = refs.pop(0), refs.pop(0)
    else:
        state_in = [refs.pop(0) for _ in range(3)]
    if last:
        out_ref = refs.pop(0)
    else:
        state_out = [refs.pop(0) for _ in range(3)]
    kv_ref, m_ref, l_ref, acc_ref, s_ref, top_ref, cut_ref = refs
    z, y, doc = meta_ref[0], meta_ref[1], meta_ref[2].astype(jnp.float32)

    for index, row in enumerate(rows):
        for place, offset in enumerate(OFFSETS):
            at = lax.rem(y + offset, Y)
            slot = index * Y + at
            a = a_refs[index]
            base = place * (PART_A + IDS)
            kv_ref[slot, 0:PART_A, :] = a[base : base + PART_A, :]
            kv_ref[slot, PART_A:, :] = b_refs[place][index * PART_B : (index + 1) * PART_B, :]
            ids = a[base + PART_A : base + PART_A + 16, :].astype(jnp.float32)[0:2, :]
            cut = jnp.sum((ids < doc).astype(jnp.int32))
            earlier = (at < y) if row == 0 else (z >= row)
            cut_ref[slot] = jnp.where(earlier, cut, ROWS)

    if first:
        own_block(
            q_ref,
            lambda: kv_ref[y, 0:ROWS, :],
            lambda: jnp.concatenate([kv_ref[y, ROWS : ROWS + 128, :], kv_ref[y, ROWS + 128 :, :]], axis=1),
            low_ref,
            own_ref,
            m_ref,
            l_ref,
            acc_ref,
        )
    else:
        m_ref[...] = state_in[0][...]
        l_ref[...] = state_in[1][...]
        acc_ref[...] = state_in[2][...]

    chunk = functools.partial(
        fold_chunk, q_ref=q_ref, kv_ref=kv_ref, m_ref=m_ref, l_ref=l_ref, acc_ref=acc_ref, s_ref=s_ref, top_ref=top_ref
    )

    def one_row(index, _):
        cuts = [cut_ref[index * Y + g] for g in range(Y)]
        total = cuts[0] + cuts[1] + cuts[2] + cuts[3]

        @pl.when(total == 0)
        def _():
            chunk(index * Y, 4, None)

        @pl.when(total > 0)
        def _():
            def one_pair(pair, _):
                slot = index * Y + 2 * pair
                low, high = cut_ref[slot], cut_ref[slot + 1]

                @pl.when(low + high < 2 * ROWS)
                def _():
                    chunk(slot, 2, (low, high))

                return 0

            lax.fori_loop(0, 2, one_pair, 0)

        return 0

    lax.fori_loop(0, len(rows), one_row, 0)

    if last:
        for tile in range(TILES):
            total = jnp.sum(l_ref[tile], axis=0, keepdims=True)
            done = (acc_ref[tile] * (1.0 / total)).T.astype(jnp.bfloat16)
            for head in range(HEADS):
                out_ref[tile, :, head * HEAD : (head + 1) * HEAD] = done[head * TILE : (head + 1) * TILE, :]
    else:
        state_out[0][...] = m_ref[...]
        state_out[1][...] = l_ref[...]
        state_out[2][...] = acc_ref[...]


STATE = (
    ((TILES, 1, COLS), jnp.float32),
    ((TILES, 8, COLS), jnp.float32),
    ((TILES, HEAD, COLS), jnp.float32),
)


def stage(rows, first, last, meta, q, a_rows, b_columns, extra, name):
    vmem = pl.BlockSpec(memory_space=pltpu.VMEM)
    if last:
        out_shape = jax.ShapeDtypeStruct((TILES, TILE, HEADS * HEAD), jnp.bfloat16)
    else:
        out_shape = tuple(jax.ShapeDtypeStruct(*s) for s in STATE)
    operands = (q, *a_rows, *b_columns, *extra)
    return pl.pallas_call(
        functools.partial(stage_kernel, rows, first, last),
        out_shape=out_shape,
        in_specs=[pl.BlockSpec(memory_space=pltpu.SMEM)] + [vmem] * len(operands),
        out_specs=vmem if last else (vmem,) * 3,
        scratch_shapes=[
            pltpu.VMEM((len(rows) * Y, 2 * ROWS, 128), jnp.bfloat16),
            *(pltpu.VMEM(*s) for s in STATE),
            pltpu.VMEM((BUFFERS, 4 * ROWS, COLS), jnp.float32),
            pltpu.VMEM((BUFFERS, 8, COLS), jnp.float32),
            pltpu.SMEM((len(rows) * Y,), jnp.int32),
        ],
        compiler_params=pltpu.CompilerParams(),
        cost_estimate=pl.CostEstimate(flops=4 * len(rows) * 10**9, bytes_accessed=4 * 2**20, transcendentals=0),
        name=name,
    )(meta, *operands)


def shift(x, dz, dy):
    pairs = [(((z + dz) % Z) * Y + (y + dy) % Y, z * Y + y) for z in range(Z) for y in range(Y)]
    return lax.ppermute(x, "ctx", pairs)


def local(queries, keys, values, segment_ids):
    here = lax.axis_index("ctx").astype(jnp.int32)
    part_a, part_b = prepare(keys.reshape(ROWS, HEAD), values.reshape(ROWS, HEAD), segment_ids.reshape(2, 128))

    q = queries.reshape(TILES, TILE, HEADS, HEAD).transpose(0, 2, 1, 3).reshape(TILES * COLS, HEAD)
    doc = segment_ids[0]
    own = (segment_ids == doc).astype(jnp.int32)
    meta = jnp.stack([here // Y, here % Y, doc])
    low = jnp.sum((segment_ids[None, :] < segment_ids[:, None]).astype(jnp.int32), axis=1)
    spread = lambda a: jnp.broadcast_to(a.reshape(TILES, 1, 1, TILE), (TILES, 1, HEADS, TILE)).reshape(TILES, 1, COLS)

    a_rows = [jnp.concatenate([part_a] + [shift(part_a, 0, offset) for offset in OFFSETS[1:]], axis=0)]
    for _ in range(4):
        a_rows.append(shift(a_rows[-1], -1, 0))
    a_rows.append(shift(a_rows[0], -5, 0))
    b_rows = [part_b]
    for _ in range(4):
        b_rows.append(shift(b_rows[-1], -1, 0))
    b_rows.append(shift(part_b, -5, 0))
    stages = ((0, 1, 2), (3, 4, 5))
    columns = []
    for rows in stages:
        column = jnp.concatenate([b_rows[r] for r in rows], axis=0)
        columns.append([column] + [shift(column, 0, offset) for offset in OFFSETS[1:]])
    state = stage(stages[0], True, False, meta, q, a_rows[:3], columns[0], (spread(low), spread(own)), "near")
    out = stage(stages[1], False, True, meta, q, a_rows[3:], columns[1], state, "far")
    out = lax.all_to_all(out, "tp", split_axis=0, concat_axis=0, tiled=True)
    return out.transpose(1, 0, 2).reshape(TILE, TILES * HEADS * HEAD)


def solution(mesh):
    in_specs = (P("ctx", "tp", None), P("ctx", "tp", None), P("ctx", "tp", None), P("ctx"))
    out_specs = P(("ctx", "tp"), None)
    return jax.shard_map(local, mesh=mesh, in_specs=in_specs, out_specs=out_specs, check_vma=False)
```

```python
import functools
import math

import jax
import jax.numpy as jnp
from jax import lax
from jax.experimental import pallas as pl
from jax.experimental.pallas import tpu as pltpu
from jax.sharding import PartitionSpec as P

Z, Y = 8, 4
ROWS = 256
HEADS = 8
HEAD = 128
TILE = 32
TILES = ROWS // TILE
COLS = TILE * HEADS
FACTOR = math.log2(math.e) / math.sqrt(HEAD)
NEG = -1e30
PART_A = 192
PART_B = 2 * ROWS - PART_A
IDS = 16
OFFSETS = (0, 1, 3, 2)
BUFFERS = 4


def prepare_kernel(k_ref, v_ref, ids_ref, a_ref, b_ref):
    a_ref[0:PART_A, :] = k_ref[0:PART_A, :]
    a_ref[PART_A : PART_A + 8, :] = jnp.zeros((8, 128), jnp.bfloat16)
    a_ref[PART_A + 8 : PART_A + 16, :] = jnp.zeros((8, 128), jnp.bfloat16)
    a_ref[PART_A : PART_A + 2, :] = ids_ref[...].astype(jnp.float32).astype(jnp.bfloat16)
    b_ref[0 : ROWS - PART_A, :] = k_ref[PART_A:ROWS, :]
    for half in range(2):
        at = ROWS - PART_A + half * 128
        v = v_ref[half * 128 : (half + 1) * 128, :].astype(jnp.float32)
        b_ref[at : at + 128, :] = v.T.astype(jnp.bfloat16)


def prepare(k, v, ids):
    vmem = pl.BlockSpec(memory_space=pltpu.VMEM)
    return pl.pallas_call(
        prepare_kernel,
        out_shape=(
            jax.ShapeDtypeStruct((PART_A + IDS, 128), jnp.bfloat16),
            jax.ShapeDtypeStruct((PART_B, 128), jnp.bfloat16),
        ),
        in_specs=[vmem] * 3,
        out_specs=(vmem, vmem),
        compiler_params=pltpu.CompilerParams(vmem_limit_bytes=4 * 2**20),
        name="prepare",
    )(k, v, ids)


def fold_chunk(first_slot, blocks, cuts, q_ref, kv_ref, m_ref, l_ref, acc_ref, s_ref, top_ref):
    length = blocks * ROWS
    carried = {}

    def scores(tile):
        q = q_ref[tile * COLS : (tile + 1) * COLS, :]
        part = None
        for g in range(blocks):
            keys = kv_ref[first_slot + g, 0:ROWS, :]
            s = lax.dot_general(keys, q, (((1,), (1,)), ((), ())), preferred_element_type=jnp.float32)
            if cuts is not None:
                row = lax.broadcasted_iota(jnp.int32, (ROWS, COLS), 0)
                s = jnp.where(row >= cuts[g], s, NEG)
            s_ref[tile % BUFFERS, g * ROWS : (g + 1) * ROWS, :] = s
            top = jnp.max(s.reshape(ROWS // 8, 8, COLS), axis=0)
            part = top if part is None else jnp.maximum(part, top)
        top_ref[tile % BUFFERS] = part

    def tops(tile):
        old = m_ref[tile]
        top = jnp.maximum(old, jnp.max(top_ref[tile % BUFFERS], axis=0, keepdims=True))
        m_ref[tile] = top
        carried[tile] = top, jnp.exp2((old - top) * FACTOR)

    def mix(tile):
        top, decay = carried.pop(tile)
        weights = jnp.exp2((s_ref[tile % BUFFERS, 0:length, :] - top) * FACTOR)
        values_t = jnp.concatenate(
            [kv_ref[first_slot + g, ROWS + h * 128 : ROWS + (h + 1) * 128, :] for g in range(blocks) for h in range(2)],
            axis=1,
        )
        mixed = jnp.dot(values_t, weights.astype(jnp.bfloat16), preferred_element_type=jnp.float32)
        l_ref[tile] = l_ref[tile] * decay + jnp.sum(weights.reshape(length // 8, 8, COLS), axis=0)
        acc_ref[tile] = acc_ref[tile] * decay + mixed

    for step in range(TILES + 2):
        if step < TILES:
            scores(step)
        if 0 <= step - 1 < TILES:
            tops(step - 1)
        if 0 <= step - 2 < TILES:
            mix(step - 2)


def own_block(q_ref, k_of, vt_of, low_ref, own_ref, m_ref, l_ref, acc_ref):
    row = lax.broadcasted_iota(jnp.int32, (ROWS, COLS), 0)
    column = lax.broadcasted_iota(jnp.int32, (1, COLS), 1)
    for tile in range(TILES):
        token = tile * TILE + lax.rem(column, TILE)
        q = q_ref[tile * COLS : (tile + 1) * COLS, :]
        s = lax.dot_general(k_of(), q, (((1,), (1,)), ((), ())), preferred_element_type=jnp.float32)
        s = jnp.where((row >= low_ref[tile]) & (row <= token), s, NEG)
        top = jnp.max(s, axis=0, keepdims=True)
        weights = jnp.exp2((s - top) * FACTOR)
        l_ref[tile] = jnp.sum(weights.reshape(ROWS // 8, 8, COLS), axis=0)
        acc_ref[tile] = jnp.dot(vt_of(), weights.astype(jnp.bfloat16), preferred_element_type=jnp.float32)
        m_ref[tile] = jnp.where(own_ref[tile] == 1, top, -NEG)


def stage_kernel(rows, first, last, *refs):
    refs = list(refs)
    meta_ref, q_ref = refs.pop(0), refs.pop(0)
    a_refs = [refs.pop(0) for _ in rows]
    b_refs = [refs.pop(0) for _ in OFFSETS]
    if first:
        low_ref, own_ref = refs.pop(0), refs.pop(0)
    else:
        state_in = [refs.pop(0) for _ in range(3)]
    if last:
        out_ref = refs.pop(0)
    else:
        state_out = [refs.pop(0) for _ in range(3)]
    kv_ref, m_ref, l_ref, acc_ref, s_ref, top_ref, cut_ref = refs
    z, y, doc = meta_ref[0], meta_ref[1], meta_ref[2].astype(jnp.float32)

    for index, row in enumerate(rows):
        for place, offset in enumerate(OFFSETS):
            at = lax.rem(y + offset, Y)
            slot = index * Y + at
            a = a_refs[index]
            base = place * (PART_A + IDS)
            kv_ref[slot, 0:PART_A, :] = a[base : base + PART_A, :]
            kv_ref[slot, PART_A:, :] = b_refs[place][index * PART_B : (index + 1) * PART_B, :]
            ids = a[base + PART_A : base + PART_A + 16, :].astype(jnp.float32)[0:2, :]
            cut = jnp.sum((ids < doc).astype(jnp.int32))
            earlier = (at < y) if row == 0 else (z >= row)
            cut_ref[slot] = jnp.where(earlier, cut, ROWS)

    if first:
        own_block(
            q_ref,
            lambda: kv_ref[y, 0:ROWS, :],
            lambda: jnp.concatenate([kv_ref[y, ROWS : ROWS + 128, :], kv_ref[y, ROWS + 128 :, :]], axis=1),
            low_ref,
            own_ref,
            m_ref,
            l_ref,
            acc_ref,
        )
    else:
        m_ref[...] = state_in[0][...]
        l_ref[...] = state_in[1][...]
        acc_ref[...] = state_in[2][...]

    chunk = functools.partial(
        fold_chunk, q_ref=q_ref, kv_ref=kv_ref, m_ref=m_ref, l_ref=l_ref, acc_ref=acc_ref, s_ref=s_ref, top_ref=top_ref
    )

    def one_row(index, _):
        cuts = [cut_ref[index * Y + g] for g in range(Y)]
        total = cuts[0] + cuts[1] + cuts[2] + cuts[3]

        @pl.when(total == 0)
        def _():
            chunk(index * Y, 4, None)

        @pl.when(total > 0)
        def _():
            def one_pair(pair, _):
                slot = index * Y + 2 * pair
                low, high = cut_ref[slot], cut_ref[slot + 1]

                @pl.when(low + high < 2 * ROWS)
                def _():
                    chunk(slot, 2, (low, high))

                return 0

            lax.fori_loop(0, 2, one_pair, 0)

        return 0

    lax.fori_loop(0, len(rows), one_row, 0)

    if last:
        for tile in range(TILES):
            total = jnp.sum(l_ref[tile], axis=0, keepdims=True)
            done = (acc_ref[tile] * (1.0 / total)).T.astype(jnp.bfloat16)
            for head in range(HEADS):
                out_ref[tile, :, head * HEAD : (head + 1) * HEAD] = done[head * TILE : (head + 1) * TILE, :]
    else:
        state_out[0][...] = m_ref[...]
        state_out[1][...] = l_ref[...]
        state_out[2][...] = acc_ref[...]


STATE = (
    ((TILES, 1, COLS), jnp.float32),
    ((TILES, 8, COLS), jnp.float32),
    ((TILES, HEAD, COLS), jnp.float32),
)


def stage(rows, first, last, meta, q, a_rows, b_columns, extra, name):
    vmem = pl.BlockSpec(memory_space=pltpu.VMEM)
    if last:
        out_shape = jax.ShapeDtypeStruct((TILES, TILE, HEADS * HEAD), jnp.bfloat16)
    else:
        out_shape = tuple(jax.ShapeDtypeStruct(*s) for s in STATE)
    operands = (q, *a_rows, *b_columns, *extra)
    return pl.pallas_call(
        functools.partial(stage_kernel, rows, first, last),
        out_shape=out_shape,
        in_specs=[pl.BlockSpec(memory_space=pltpu.SMEM)] + [vmem] * len(operands),
        out_specs=vmem if last else (vmem,) * 3,
        scratch_shapes=[
            pltpu.VMEM((len(rows) * Y, 2 * ROWS, 128), jnp.bfloat16),
            *(pltpu.VMEM(*s) for s in STATE),
            pltpu.VMEM((BUFFERS, 4 * ROWS, COLS), jnp.float32),
            pltpu.VMEM((BUFFERS, 8, COLS), jnp.float32),
            pltpu.SMEM((len(rows) * Y,), jnp.int32),
        ],
        compiler_params=pltpu.CompilerParams(vmem_limit_bytes=24 * 2**20),
        cost_estimate=pl.CostEstimate(flops=4 * len(rows) * 10**9, bytes_accessed=4 * 2**20, transcendentals=0),
        name=name,
    )(meta, *operands)


def shift(x, dz, dy):
    pairs = [(((z + dz) % Z) * Y + (y + dy) % Y, z * Y + y) for z in range(Z) for y in range(Y)]
    return lax.ppermute(x, "ctx", pairs)


def local(queries, keys, values, segment_ids):
    here = lax.axis_index("ctx").astype(jnp.int32)
    part_a, part_b = prepare(keys.reshape(ROWS, HEAD), values.reshape(ROWS, HEAD), segment_ids.reshape(2, 128))

    q = queries.reshape(TILES, TILE, HEADS, HEAD).transpose(0, 2, 1, 3).reshape(TILES * COLS, HEAD)
    doc = segment_ids[0]
    own = (segment_ids == doc).astype(jnp.int32)
    meta = jnp.stack([here // Y, here % Y, doc])
    low = jnp.sum((segment_ids[None, :] < segment_ids[:, None]).astype(jnp.int32), axis=1)
    spread = lambda a: jnp.broadcast_to(a.reshape(TILES, 1, 1, TILE), (TILES, 1, HEADS, TILE)).reshape(TILES, 1, COLS)

    a_rows = [jnp.concatenate([part_a] + [shift(part_a, 0, offset) for offset in OFFSETS[1:]], axis=0)]
    for _ in range(4):
        a_rows.append(shift(a_rows[-1], -1, 0))
    a_rows.append(shift(a_rows[0], -5, 0))
    b_rows = [part_b]
    for _ in range(4):
        b_rows.append(shift(b_rows[-1], -1, 0))
    b_rows.append(shift(part_b, -5, 0))
    stages = ((0, 1, 2), (3, 4, 5))
    columns = []
    for rows in stages:
        column = jnp.concatenate([b_rows[r] for r in rows], axis=0)
        columns.append([column] + [shift(column, 0, offset) for offset in OFFSETS[1:]])
    state = stage(stages[0], True, False, meta, q, a_rows[:3], columns[0], (spread(low), spread(own)), "near")
    out = stage(stages[1], False, True, meta, q, a_rows[3:], columns[1], state, "far")
    out = lax.all_to_all(out, "tp", split_axis=0, concat_axis=0, tiled=True)
    return out.transpose(1, 0, 2).reshape(TILE, TILES * HEADS * HEAD)


def solution(mesh):
    in_specs = (P("ctx", "tp", None), P("ctx", "tp", None), P("ctx", "tp", None), P("ctx"))
    out_specs = P(("ctx", "tp"), None)
    return jax.shard_map(local, mesh=mesh, in_specs=in_specs, out_specs=out_specs, check_vma=False)
```
